32 devices in a mesh: section: 4 (over x, core), wide: 8 (over z, y).
Axes of the slice: x: 2, y: 2, z: 4, core: 2. Of those that a mesh axis runs over, the one named last changes fastest.
Arguments:
- stream: bfloat16 [4, 512, 2048], P('section', 'wide'), may hold values from -3 to 3
- mixer_gain: float32 [4, 2048], P('section'), may hold values from 0.1 to 1.9
- ssm_weight: bfloat16 [4, 2048, 160], P('section'), may hold values from -0.125 to 0.125
- decay_rate: float32 [4, 32], P('section'), may hold values from 9.765625e-05 to 0.04
- skip_gain: float32 [4, 32], P('section'), may hold values from 0.5 to 1.5
- mixed_gain: float32 [4, 2048], P('section'), may hold values from 0.1 to 1.9
- ffn_gain: float32 [4, 2048], P('section'), may hold values from 0.1 to 1.9
- router_weight: bfloat16 [4, 2048, 4], P('section'), may hold values from -0.125 to 0.125
- expert_ids: int32 [4, 512, 2], P('section', 'wide'), may hold values from 0 to 3, all different within a row; in each aligned block of 64 rows (0 to 63, 64 to 127, ..., all dimensions but the last counted through in order) at most 40 rows name the same one
- gate_weight: bfloat16 [4, 2048, 28672], P('section', None, 'wide'), may hold values from -0.125 to 0.125
- up_weight: bfloat16 [4, 2048, 28672], P('section', None, 'wide'), may hold values from -0.125 to 0.125
- down_weight: bfloat16 [4, 28672, 2048], P('section', 'wide'), may hold values from -0.0625 to 0.0625
Outputs:
- carried: bfloat16 [4, 512, 2048], P('section', 'wide')
The draws below stay inside these ranges and needn't reach their ends.
Inputs may be any that keep to these rules, and one draw needn't show every extreme that they name: `expert_ids`: A token's 2 experts differ. Among the tokens of one device, no expert is named by more than 40 of them, a bound that some block reaches.
All inputs are finite; a program needn't handle non-finite values.
Results may differ from the reference program's by a relative error of at most 0.0085.
Values may be sent and summed in bfloat16 or wider, within the bound.
A program may use at most 128 MiB of HBM per device.

```python
import math
import jax
import jax.numpy as jnp
import numpy as np
from jax import lax

D = 2048
HEADS = 32
HEAD_DIM = 64
STATE = 64
EXPERTS = 4
FF = 7168
TOP = 2
TOK_DEV = 64
CAP = 40
TOKENS = 512
SECTIONS = 4
N_WIDE = 8


def level_of(stream_key, dims, split, low, largest):
    factor_of, own = 1.0, jax.random.fold_in(stream_key, 6)
    for axis_at, shards_of in split:
        draws = jnp.exp(jax.random.uniform(jax.random.fold_in(own, axis_at), (shards_of,), jnp.float32, low / len(split), largest / len(split)))
        factor_of = factor_of * jnp.repeat(draws, dims[axis_at] // shards_of).reshape([-1 if axis == axis_at else 1 for axis in range(len(dims))])
    return factor_of


def shared_out(rng, own, number, rows, count, top, limit, lean):
    sequence = jax.random.permutation(rng, count)
    heavy_load, common = portions_of(count, rows * top, limit, lean, True), portions_of(count, rows * top, limit, lean, False)
    places = jnp.arange(count)

    def named(tallies, rotation):
        used = int((tallies > 0).sum())
        fixed = max(1, used // 4)
        passed = fixed + (places - fixed + rotation * (used - fixed)) % max(1, count - fixed)
        return jnp.zeros((count,), jnp.int32).at[sequence[jnp.where(places < fixed, places, passed)]].set(jnp.asarray(tallies, jnp.int32))

    tallies = jnp.where(number % 4 == 0, named(heavy_load, number // 4), named(common, number - number // 4 - 1))
    mixed = jax.random.permutation(jax.random.fold_in(own, 3), count)
    source_of, sink = mixed[0:count // 2 * 2:2], mixed[1:count // 2 * 2:2]
    slack = jnp.minimum(tallies[source_of] - 1, limit - tallies[sink]) // 2
    slack = jnp.where((source_of == sequence[0]) | (sink == sequence[0]) | (tallies[sink] == 0), 0, jnp.maximum(slack, 0))
    passed = jax.random.randint(jax.random.fold_in(own, 4), (count // 2,), 0, 1 << 20) % (slack + 1)
    tallies = tallies.at[source_of].add(-passed).at[sink].add(passed)
    labels = jnp.searchsorted(jnp.cumsum(tallies), jnp.arange(rows * top), side="right").astype(jnp.int32)
    table = labels.reshape(top, rows).T
    table = table[jax.random.permutation(jax.random.fold_in(own, 1), rows)]
    rotation = jax.random.randint(jax.random.fold_in(own, 2), (rows, 1), 0, top)
    return jnp.take_along_axis(table, (jnp.arange(top)[None, :] + rotation) % top, axis=1)


def portions_of(amount, total, bound, skew, full):
    loads = [(1 << 20) // math.isqrt(grade ** skew) + 1 for grade in range(1, amount + 1)]
    largest = bound if full else min(bound, max(-(-total // amount), total * loads[0] // sum(loads)))
    least = 1 if total - largest >= amount - 1 else 0
    counts, rest = [largest] + [least] * (amount - 1), total - largest - least * (amount - 1)
    while rest > 0:
        movable = [i for i in range(1, amount) if counts[i] < largest] or [i for i in range(1, amount) if counts[i] < bound]
        whole, remaining = sum([loads[i] for i in movable]), rest
        for i in movable:
            extra = min(bound - counts[i], max(1, remaining * loads[i] // whole), rest)
            counts[i] = counts[i] + extra
            rest = rest - extra
    return np.array(counts)


def bell_draw(rng, extent, spread, most, split=(), held_as=jnp.bfloat16):
    result = spread * jax.random.normal(rng, extent, jnp.float32)
    if split:
        result = result * level_of(rng, extent, split, -0.22, 0.18)
    return jnp.clip(result, -most, most).astype(held_as)


def setup_inputs(seed: int = 0) -> dict:
    seeds = jax.random.split(jax.random.key(seed), 13)
    stream = bell_draw(seeds[0], (SECTIONS, TOKENS, D), 0.5, 3.0, ((0, 4), (1, 8)))
    mixer_gain = jnp.clip(1.0 + 0.18 * jax.random.normal(seeds[1], (SECTIONS, D), jnp.float32), 0.1, 1.9)
    ssm_weight = bell_draw(seeds[2], (SECTIONS, D, 2 * STATE + HEADS), D ** -0.5, 0.125, ((0, 4),))
    decay_rate = jnp.clip(jnp.exp(math.log(0.04) - 6.015181 * jax.random.uniform(seeds[3], (SECTIONS, HEADS), jnp.float32) ** level_of(seeds[3], (SECTIONS, HEADS), ((0, 4),), -0.2, 0.2)), 9.765625145519152e-05, 0.04)
    skip_gain = jnp.clip(0.5 + 1.0 * jax.random.uniform(seeds[4], (SECTIONS, HEADS), jnp.float32) ** level_of(seeds[4], (SECTIONS, HEADS), ((0, 4),), -0.2, 0.2), 0.5, 1.5)
    mixed_gain = jnp.clip(1.0 + 0.18 * jax.random.normal(seeds[5], (SECTIONS, D), jnp.float32), 0.1, 1.9)
    ffn_gain = jnp.clip(1.0 + 0.18 * jax.random.normal(seeds[6], (SECTIONS, D), jnp.float32), 0.1, 1.9)
    router_weight = bell_draw(seeds[7], (SECTIONS, D, EXPERTS), D ** -0.5, 0.125, ((0, 4),))
    expert_ids_keys = jax.random.split(jax.random.fold_in(seeds[8], 1), SECTIONS * TOKENS // TOK_DEV)
    expert_ids_turns = jax.random.permutation(jax.random.fold_in(seeds[8], 3), SECTIONS * TOKENS // TOK_DEV)
    expert_ids = jax.vmap(lambda own, number: shared_out(jax.random.fold_in(seeds[8], 2), own, number, TOK_DEV, EXPERTS, TOP, CAP, 2))(expert_ids_keys, expert_ids_turns).reshape((SECTIONS, TOKENS, TOP))
    gate_weight = bell_draw(seeds[9], (SECTIONS, D, EXPERTS * FF), D ** -0.5, 0.125, ((0, 4), (2, 8)))
    up_weight = bell_draw(seeds[10], (SECTIONS, D, EXPERTS * FF), D ** -0.5, 0.125, ((0, 4), (2, 8)))
    down_weight = bell_draw(seeds[11], (SECTIONS, EXPERTS * FF, D), FF ** -0.5, 0.0625, ((0, 4), (1, 8)))
    return dict(stream=stream, mixer_gain=mixer_gain, ssm_weight=ssm_weight, decay_rate=decay_rate, skip_gain=skip_gain, mixed_gain=mixed_gain, ffn_gain=ffn_gain, router_weight=router_weight, expert_ids=expert_ids, gate_weight=gate_weight, up_weight=up_weight, down_weight=down_weight)


EPSILON = 1e-05
HIGHEST_PREC = lax.Precision.HIGHEST

def rms_scale(values, gain_row):
    mean_sq = lax.optimization_barrier(jnp.mean(values * values, axis=-1, keepdims=True))
    return values * lax.rsqrt(mean_sq + EPSILON) * gain_row

def route_slots(id_rows):
    flat_ids = id_rows.reshape(-1).astype(jnp.int32)
    one_hot = (flat_ids[:, None] == jnp.arange(EXPERTS, dtype=jnp.int32)[None, :]).astype(jnp.int32)
    running = jnp.cumsum(one_hot, axis=0) - 1
    slot_ids = lax.optimization_barrier(jnp.sum(one_hot * running, axis=1)).astype(jnp.int32)
    return flat_ids * CAP + slot_ids

def mixer_block(inputs, mixer_gain, ssm_weight, decay_rate, skip_gain, mixed_gain):
    residual = inputs.astype(jnp.float32)
    normed = rms_scale(residual, mixer_gain).astype(jnp.bfloat16)
    projected = jnp.dot(normed, ssm_weight, preferred_element_type=jnp.float32)
    b_rows = projected[:, :STATE] / float(STATE)
    c_rows = projected[:, STATE:2 * STATE] / math.sqrt(STATE)
    step_size = jax.nn.softplus(projected[:, 2 * STATE:])
    values = normed.astype(jnp.float32)
    decay_cols = jnp.repeat(jnp.exp(-step_size * decay_rate[None, :]), HEAD_DIM, axis=1)
    step_cols = jnp.repeat(step_size, HEAD_DIM, axis=1)

    def advance(carry_state, inputs_row):
        decay_row, step_row, b_row, c_row, value_row = inputs_row
        carry_state = decay_row[None, :] * carry_state + b_row[:, None] * (step_row * value_row)[None, :]
        return (carry_state, jnp.dot(c_row, carry_state, precision=HIGHEST_PREC))
    start_state = jnp.zeros((STATE, D), jnp.float32)
    _, readout = lax.scan(advance, start_state, (decay_cols, step_cols, b_rows, c_rows, values))
    mixed = readout + values * jnp.repeat(skip_gain, HEAD_DIM)[None, :]
    return residual + rms_scale(mixed, mixed_gain)

def expert_layer(residual, ffn_gain, router_weight, id_rows, gate_weight, up_weight, down_weight):
    routed = rms_scale(residual, ffn_gain).astype(jnp.bfloat16)
    logits = jnp.dot(routed, router_weight, preferred_element_type=jnp.float32)
    chosen = jnp.take_along_axis(logits, id_rows, axis=1)
    first_share = jax.nn.sigmoid(chosen[:, 0] - chosen[:, 1])
    shares = jnp.stack([first_share, 1.0 - first_share], axis=1)
    blocks = id_rows.reshape(N_WIDE, TOK_DEV, TOP)
    targets = jax.vmap(route_slots)(blocks)
    experts_of = blocks.reshape(N_WIDE, TOK_DEV * TOP).astype(jnp.int32)
    offsets = (jnp.arange(N_WIDE, dtype=jnp.int32) * CAP)[:, None]
    rows_at = (targets - experts_of * CAP + offsets).reshape(-1)
    experts_flat = experts_of.reshape(-1)
    doubled = jnp.repeat(routed, TOP, axis=0)
    buffers = jnp.zeros((EXPERTS, N_WIDE * CAP, D), jnp.bfloat16).at[experts_flat, rows_at].set(doubled)
    members = N_WIDE // EXPERTS
    part_width = FF // members
    gate_all = gate_weight.reshape(D, EXPERTS, FF).transpose(1, 0, 2)
    up_all = up_weight.reshape(D, EXPERTS, FF).transpose(1, 0, 2)
    down_all = down_weight.reshape(EXPERTS, FF, D)

    def one_expert(pieces):
        rows_in, gate_one, up_one, down_one = pieces
        gate_pre = jnp.dot(rows_in, gate_one, preferred_element_type=jnp.float32)
        up_pre = jnp.dot(rows_in, up_one, preferred_element_type=jnp.float32)
        hidden = (jax.nn.silu(gate_pre) * up_pre).astype(jnp.bfloat16)
        split_hidden = hidden.reshape(-1, members, part_width).astype(jnp.float32)
        split_down = down_one.reshape(members, part_width, D).astype(jnp.float32)
        partials = jnp.einsum('rgf,gfd->grd', split_hidden, split_down, precision=HIGHEST_PREC)
        return lax.optimization_barrier(jnp.sum(partials.astype(jnp.bfloat16).astype(jnp.float32), axis=0))
    answers = lax.map(one_expert, (buffers, gate_all, up_all, down_all))
    picked = answers[experts_flat, rows_at].reshape(TOKENS, TOP, D)
    return (residual + lax.optimization_barrier(jnp.sum(picked * shares[:, :, None], axis=1))).astype(jnp.bfloat16)

def reference(stream, mixer_gain, ssm_weight, decay_rate, skip_gain, mixed_gain, ffn_gain, router_weight, expert_ids, gate_weight, up_weight, down_weight):
    outputs = []
    for section_index in range(SECTIONS):
        residual = mixer_block(stream[section_index], mixer_gain[section_index], ssm_weight[section_index], decay_rate[section_index], skip_gain[section_index], mixed_gain[section_index])
        outputs.append(expert_layer(residual, ffn_gain[section_index], router_weight[section_index], expert_ids[section_index], gate_weight[section_index], up_weight[section_index], down_weight[section_index]))
    return jnp.roll(jnp.stack(outputs), 1, axis=0)
```

```python
import functools
import math

import jax
import jax.numpy as jnp
from jax import lax
from jax.experimental import pallas as pl
from jax.experimental.pallas import tpu as pltpu
from jax.sharding import PartitionSpec as P

STATE = 64
EXPERTS = 4
CAP = 40
EPSILON = 1e-05
PIECES = 8
CUTS = 2
VMEM_BYTES = 67_000_000
F32 = jnp.float32
BF16 = jnp.bfloat16


def tile_of(extent, most):
    return max(t for t in range(128, most + 1, 128) if extent % t == 0)


def rms_scale(values, gain_row):
    mean_sq = jnp.mean(values * values, axis=-1, keepdims=True)
    return values * lax.rsqrt(mean_sq + EPSILON) * gain_row


def iota(shape, axis):
    return lax.broadcasted_iota(jnp.int32, shape, axis)


def dot(a, b):
    return jnp.dot(a, b, preferred_element_type=F32)


def split_pair(values):
    high = values.astype(BF16).astype(F32)
    return jnp.concatenate([high, values - high], axis=1)


def tick(
    sections,
    n,
    stream,
    mixer_gain,
    ssm_weight,
    decay_rate,
    skip_gain,
    mixed_gain,
    ffn_gain,
    router_weight,
    expert_ids,
    gate_hbm,
    up_hbm,
    down_hbm,
    out_ref,
    gate,
    up,
    down,
    local_out,
    local_in,
    decay_out,
    decay_in,
    start_out,
    start_in,
    mixed,
    carry,
    resid,
    notes,
    resid_in,
    notes_in,
    packed,
    arrived,
    rows_in,
    hidden,
    answers,
    shared_in,
    totals,
    answers_in,
    picked,
    w_sem,
    local_send,
    local_recv,
    decay_send,
    decay_recv,
    start_send,
    start_recv,
    pass_send,
    pass_recv,
    rows_send,
    rows_recv,
    share_send,
    share_recv,
    ans_send,
    ans_recv,
):
    sec = lax.axis_index("section")
    me = lax.axis_index("wide")
    after = lax.rem(sec + 1, sections)
    before = lax.rem(sec + sections - 1, sections)
    tok, width = stream.shape
    heads = decay_rate.shape[1]
    head_dim = width // heads
    assert tok == head_dim
    chans = width // n
    members = n // EXPERTS
    my_expert, my_part = me // members, lax.rem(me, members)
    hid = gate.shape[1]
    order = [0]
    for k in range(1, n // 2 + 1):
        order += [k] if 2 * k == n else [k, n - k]

    def wide_at(shift):
        return lax.rem(me + (shift + n), n)

    mates = [
        my_expert,
        my_expert + 1 - 2 * lax.rem(my_expert, 2),
        lax.rem(my_expert + 2, EXPERTS),
        EXPERTS - 1 - my_expert,
    ]

    def peer(q, part_shift):
        return mates[q] * members + lax.rem(my_part + (part_shift + members), members)

    def remote(src, dst, send, recv, section, wide):
        return pltpu.make_async_remote_copy(
            src_ref=src,
            dst_ref=dst,
            send_sem=send,
            recv_sem=recv,
            device_id={"section": section, "wide": wide},
            device_id_type=pl.DeviceIdType.MESH,
        )

    barrier = pltpu.get_barrier_semaphore()
    for k in range(n):
        w = wide_at(k)
        if k:
            pl.semaphore_signal(
                barrier, inc=1, device_id={"section": sec, "wide": w},
                device_id_type=pl.DeviceIdType.MESH,
            )
        for other in (after, before):
            pl.semaphore_signal(
                barrier, inc=1, device_id={"section": other, "wide": w},
                device_id_type=pl.DeviceIdType.MESH,
            )

    weight_copies = []
    for i, (src, dst) in enumerate(((gate_hbm, gate), (up_hbm, up), (down_hbm, down))):
        step = src.shape[0] // PIECES
        weight_copies.append(
            [
                pltpu.make_async_copy(
                    src.at[pl.ds(k * step, step)], dst.at[pl.ds(k * step, step)], w_sem.at[i, k]
                )
                for k in range(PIECES)
            ]
        )
        for copy in weight_copies[-1]:
            copy.start()

    x_in = stream[...].astype(F32)
    normed = rms_scale(x_in, mixer_gain[...]).astype(BF16)
    projected = lax.dot_general(
        normed, ssm_weight[...], (((1,), (1,)), ((), ())), preferred_element_type=F32
    )
    raw = projected[:, 2 * STATE :]
    step_size = jnp.maximum(raw, 0.0) + jnp.log1p(jnp.exp(-jnp.abs(raw)))
    b_rows = projected[:, :STATE] * (1.0 / STATE)
    c_rows = (projected[:, STATE : 2 * STATE] * (1.0 / math.sqrt(STATE))).astype(BF16)
    tri = (iota((tok, tok), 0) >= iota((tok, tok), 1)).astype(BF16)
    steps = split_pair(step_size)
    run = dot(tri, steps.astype(BF16))
    rated = (run[:, :heads] + run[:, heads:]) * decay_rate[...]
    skips = jnp.broadcast_to(split_pair(skip_gain[...]), (16, 2 * heads))
    spread = (
        lax.rem(iota((2 * heads, width), 0), heads) == iota((2 * heads, width), 1) // head_dim
    ).astype(BF16)
    cols = dot(
        jnp.concatenate([steps, split_pair(rated), skips], axis=0).astype(BF16), spread
    )
    step_cols, rated_cols = cols[:tok], cols[tok : 2 * tok]
    skip_cols = cols[2 * tok : 2 * tok + 1]
    values = normed.astype(F32)
    scaled = values * step_cols
    last = rated_cols[tok - 1 : tok]

    b_across = jnp.transpose(b_rows).astype(BF16)
    added = dot(b_across, (scaled * jnp.exp(rated_cols - last)).astype(BF16)).astype(BF16)
    faded = jnp.exp(-last)
    for j in range(n):
        at = slice(j * chans, (j + 1) * chans)
        local_out[j] = added[:, at]
        decay_out[j] = faded[:, at]
    pl.semaphore_wait(barrier, 3 * n - 1)
    own_copies = [
        pltpu.make_async_copy(local_out.at[me], local_in.at[me], local_recv.at[me]),
        pltpu.make_async_copy(decay_out.at[me], decay_in.at[me], decay_recv.at[me]),
    ]
    for copy in own_copies:
        copy.start()
    for p in reversed(range(1, n)):
        w = wide_at(order[p])
        remote(
            decay_out.at[w], decay_in.at[me], decay_send.at[w], decay_recv.at[me], sec, w
        ).start()
        remote(
            local_out.at[w], local_in.at[me], local_send.at[w], local_recv.at[me], sec, w
        ).start()

    per = 256 // head_dim
    block = per * head_dim
    b_short = b_rows.astype(BF16)
    overlap = lax.dot_general(
        c_rows, jnp.concatenate([b_rows] * per, axis=0).astype(BF16),
        (((1,), (1,)), ((), ())), preferred_element_type=F32,
    )
    lane_tok = lax.rem(iota((tok, block), 1), tok)
    lane_head = iota((tok, block), 1) // head_dim
    row_tok = iota((tok, block), 0)
    for g in range(width // block):
        at = slice(g * block, (g + 1) * block)
        rated_g, scaled_g = rated_cols[:, at], scaled[:, at]
        rated_row = jnp.sum(
            jnp.where(row_tok == lane_tok, rated_g, 0.0), axis=0, keepdims=True
        )
        gap = jnp.where(row_tok >= lane_tok, rated_row - rated_g, -1e30)
        mixing = (overlap * jnp.exp(gap)).astype(BF16)
        stacked = jnp.concatenate(
            [jnp.where(lane_head == k, scaled_g, 0.0) for k in range(per)], axis=0
        ).astype(BF16)
        mixed[:, at] = dot(mixing, stacked) + values[:, at] * skip_cols[:, at]
        carry[:, at] = jnp.exp(-rated_g)

    for copy in own_copies:
        copy.wait()
    for p in range(1, n):
        w = wide_at(order[p])
        remote(
            decay_out.at[w], decay_in.at[w], decay_send.at[w], decay_recv.at[w], sec, w
        ).wait()
        remote(
            local_out.at[w], local_in.at[w], local_send.at[w], local_recv.at[w], sec, w
        ).wait()
    state = jnp.zeros((STATE, chans), F32)
    for w in range(n):
        start_out[w] = state.astype(BF16)
        state = state * decay_in[w] + local_in[w].astype(F32)
    start_own = pltpu.make_async_copy(start_out.at[me], start_in.at[me], start_recv.at[me])
    start_own.start()
    for p in reversed(range(1, n)):
        w = wide_at(order[p])
        remote(
            start_out.at[w], start_in.at[me], start_send.at[w], start_recv.at[me], sec, w
        ).start()

    id_rows = jnp.concatenate([expert_ids[...], jnp.zeros((6, tok), jnp.int32)], axis=0)
    ids = jnp.transpose(id_rows.astype(F32)).astype(jnp.int32)
    id0, id1 = ids[:, 0:1], ids[:, 1:2]
    lane = iota((tok, 128), 1)
    chosen = ((lane == id0) | (lane == id1)).astype(BF16)
    earlier = (iota((tok, tok), 0) > iota((tok, tok), 1)).astype(BF16)
    running = dot(earlier, chosen)
    slot0 = jnp.sum(jnp.where(lane == id0, running, 0.0), axis=1, keepdims=True)
    slot1 = jnp.sum(jnp.where(lane == id1, running, 0.0), axis=1, keepdims=True)
    target0 = id0.astype(F32) * CAP + slot0
    target1 = id1.astype(F32) * CAP + slot1
    places = iota((tok, 256), 1).astype(F32)
    placing = jnp.transpose(((places == target0) | (places == target1)).astype(F32)).astype(BF16)

    start_own.wait()
    for p in range(1, n):
        w = wide_at(order[p])
        remote(
            start_out.at[w], start_in.at[w], start_send.at[w], start_recv.at[w], sec, w
        ).wait()
    for j in range(n):
        at = slice(j * chans, (j + 1) * chans)
        mixed[:, at] = mixed[:, at] + dot(c_rows, start_in[j]) * carry[:, at]
    residual = x_in + rms_scale(mixed[...], mixed_gain[...])
    routed = rms_scale(residual, ffn_gain[...]).astype(BF16)
    sent = dot(placing[: EXPERTS * CAP], routed)
    piece = width // CUTS
    for e in range(EXPERTS):
        for c in range(CUTS):
            packed[e, c] = sent[
                e * CAP : (e + 1) * CAP, c * piece : (c + 1) * piece
            ].astype(BF16)

    row_copies = {}
    rows_own = []
    for c in range(CUTS):
        rows_own.append(
            pltpu.make_async_copy(packed.at[my_expert, c], arrived.at[0, c], rows_recv.at[0, c])
        )
        rows_own[-1].start()

    def hand_on(q, c):
        source = arrived.at[q, c] if q else packed.at[my_expert, c]
        for k in range(1, members):
            p = k * EXPERTS + q
            row_copies[p, c] = remote(
                source, arrived.at[p, c], rows_send.at[p, c], rows_recv.at[p, c], sec, peer(0, -k)
            )
            row_copies[p, c].start()

    for c in range(CUTS):
        hand_on(0, c)
    for q in (2, 3, 1):
        for c in range(CUTS):
            row_copies[q, c] = remote(
                packed.at[mates[q], c], arrived.at[q, c], rows_send.at[q, c], rows_recv.at[q, c],
                sec, peer(q, 0),
            )
            row_copies[q, c].start()

    logits = lax.dot_general(
        routed, router_weight[...], (((1,), (1,)), ((), ())), preferred_element_type=F32
    )
    choice = iota((tok, EXPERTS), 1)
    logit0 = jnp.sum(jnp.where(choice == id0, logits, 0.0), axis=1, keepdims=True)
    logit1 = jnp.sum(jnp.where(choice == id1, logits, 0.0), axis=1, keepdims=True)
    share0 = jax.nn.sigmoid(logit0 - logit1)
    resid[...] = residual
    notes[...] = jnp.where(
        lane == 0, target0, jnp.where(lane == 1, target1, jnp.where(lane == 2, share0, 0.0))
    )
    passes = [
        remote(resid, resid_in, pass_send.at[0], pass_recv.at[0], after, me),
        remote(notes, notes_in, pass_send.at[1], pass_recv.at[1], after, me),
    ]
    for copy in passes:
        copy.start()

    def relay(q):
        for c in range(CUTS):
            row_copies[q, c].wait_recv()
            hand_on(q, c)

    hid_tile = tile_of(hid, 512)
    out_tile = totals.shape[3]
    tiles = width // out_tile
    steps_up = hid // hid_tile
    groups = ((0, 2), (1, 3))
    half = n // 2
    share_copies = {}
    answer_copies = {}

    def gather(group):
        block_at = 0
        for k in range(members):
            for q in groups[group]:
                p = k * EXPERTS + q
                for c in range(CUTS):
                    if p == 0:
                        rows_own[c].wait()
                    elif k:
                        row_copies[p, c].wait_recv()
                block_at += 1
            lead = k * EXPERTS + groups[group][0]
            other = k * EXPERTS + groups[group][1]
            top = k * 2 * CAP
            for c in range(CUTS):
                rows_in[top : top + 2 * CAP, c * piece : (c + 1) * piece] = jnp.concatenate(
                    [arrived[lead, c].astype(F32), arrived[other, c].astype(F32)], axis=0
                ).astype(BF16)

    def widen(first, last_step):
        @pl.loop(first, last_step)
        def _(i):
            at = pl.ds(pl.multiple_of(i * hid_tile, hid_tile), hid_tile)
            gate_pre = dot(rows_in[...], gate[:, at])
            up_pre = dot(rows_in[...], up[:, at])
            hidden[:, at] = (gate_pre * jax.nn.sigmoid(gate_pre) * up_pre).astype(BF16)

    def narrow(group):
        for i in range(tiles):
            result = dot(hidden[...], down[:, i * out_tile : (i + 1) * out_tile])
            for k in reversed(range(members)):
                for h, q in enumerate(groups[group]):
                    p = k * EXPERTS + q
                    top = (k * 2 + h) * CAP
                    answers[p, i] = result[top : top + CAP].astype(BF16)
            for k in range(1, members):
                for q in groups[group]:
                    p = k * EXPERTS + q
                    share_copies[p, i] = remote(
                        answers.at[p, i], shared_in.at[p - EXPERTS, i],
                        share_send.at[p - EXPERTS, i], share_recv.at[p - EXPERTS, i],
                        sec, peer(0, k),
                    )
                    share_copies[p, i].start()

    def settle(group, i):
        for q in reversed(groups[group]):
            total = answers[q, i].astype(F32)
            for k in range(1, members):
                p = k * EXPERTS + q
                share_copies[p, i].wait_recv()
                total = total + shared_in[p - EXPERTS, i].astype(F32)
            totals[q, i] = total.astype(BF16)
            answer_copies[q, i] = remote(
                totals.at[q, i], answers_in.at[q, i], ans_send.at[q, i], ans_recv.at[q, i],
                after, peer(q, 0),
            )
            answer_copies[q, i].start()

    relay(2)
    relay(1)
    gather(0)
    for copies in weight_copies[:2]:
        for copy in copies:
            copy.wait()
    cut = steps_up - steps_up // 4
    widen(0, cut)
    relay(3)
    widen(cut, steps_up)
    for copy in weight_copies[2]:
        copy.wait()
    narrow(0)
    gather(1)
    cut = steps_up // 2
    widen(0, cut)
    for i in range(tiles):
        settle(0, i)
    widen(cut, steps_up)
    narrow(1)

    for copy in passes:
        copy.wait()
    told = notes_in[...]
    goal0, goal1, first_share = told[:, 0:1], told[:, 1:2], told[:, 2:3]
    slot_lane = iota((tok, CAP), 1)

    def take(q):
        spots = (slot_lane + mates[q] * CAP).astype(F32)
        return jnp.concatenate(
            [(spots == goal0).astype(F32), (spots == goal1).astype(F32)], axis=0
        ).astype(BF16)

    for i in range(tiles):
        settle(1, i)
    takes = [take(q) for q in range(EXPERTS)]
    for i in range(tiles):
        at = slice(i * out_tile, (i + 1) * out_tile)
        found = None
        for q in groups[0]:
            answer_copies[q, i].wait_recv()
            part = dot(takes[q], answers_in[q, i])
            found = part if found is None else found + part
        picked[:, at] = found
    for i in range(tiles):
        at = slice(i * out_tile, (i + 1) * out_tile)
        found = picked[:, at]
        for q in groups[1]:
            answer_copies[q, i].wait_recv()
            found = found + dot(takes[q], answers_in[q, i])
        out_ref[:, at] = (
            resid_in[:, at] + (first_share * found[:tok] + (1.0 - first_share) * found[tok:])
        ).astype(BF16)
    for p in range(1, n):
        for c in range(CUTS):
            row_copies[p, c].wait_send()
    for copy in share_copies.values():
        copy.wait_send()
    for copy in answer_copies.values():
        copy.wait_send()


def local(
    stream,
    mixer_gain,
    ssm_weight,
    decay_rate,
    skip_gain,
    mixed_gain,
    ffn_gain,
    router_weight,
    expert_ids,
    gate_weight,
    up_weight,
    down_weight,
):
    n = lax.axis_size("wide")
    sections = lax.axis_size("section")
    _, tok, width = stream.shape
    hid = gate_weight.shape[2]
    chans = width // n
    out_tile = tile_of(width, 512)
    tiles = width // out_tile
    dma = pltpu.SemaphoreType.DMA
    vmem = pl.BlockSpec(memory_space=pltpu.VMEM)
    hbm = pl.BlockSpec(memory_space=pl.ANY)
    result = pl.pallas_call(
        functools.partial(tick, sections, n),
        out_shape=jax.ShapeDtypeStruct((tok, width), BF16),
        in_specs=[vmem] * 9 + [hbm] * 3,
        out_specs=vmem,
        scratch_shapes=[
            pltpu.VMEM((width, hid), BF16),
            pltpu.VMEM((width, hid), BF16),
            pltpu.VMEM((hid, width), BF16),
            pltpu.VMEM((n, STATE, chans), BF16),
            pltpu.VMEM((n, STATE, chans), BF16),
            pltpu.VMEM((n, 1, chans), F32),
            pltpu.VMEM((n, 1, chans), F32),
            pltpu.VMEM((n, STATE, chans), BF16),
            pltpu.VMEM((n, STATE, chans), BF16),
            pltpu.VMEM((tok, width), F32),
            pltpu.VMEM((tok, width), F32),
            pltpu.VMEM((tok, width), F32),
            pltpu.VMEM((tok, 128), F32),
            pltpu.VMEM((tok, width), F32),
            pltpu.VMEM((tok, 128), F32),
            pltpu.VMEM((EXPERTS, CUTS, CAP, width // CUTS), BF16),
            pltpu.VMEM((n, CUTS, CAP, width // CUTS), BF16),
            pltpu.VMEM((n // 2 * CAP, width), BF16),
            pltpu.VMEM((n // 2 * CAP, hid), BF16),
            pltpu.VMEM((n, tiles, CAP, out_tile), BF16),
            pltpu.VMEM((n - EXPERTS, tiles, CAP, out_tile), BF16),
            pltpu.VMEM((EXPERTS, tiles, CAP, out_tile), BF16),
            pltpu.VMEM((EXPERTS, tiles, CAP, out_tile), BF16),
            pltpu.VMEM((2 * tok, width), F32),
            dma((3, PIECES)),
            dma((n,)),
            dma((n,)),
            dma((n,)),
            dma((n,)),
            dma((n,)),
            dma((n,)),
            dma((2,)),
            dma((2,)),
            dma((n, CUTS)),
            dma((n, CUTS)),
            dma((n - EXPERTS, tiles)),
            dma((n - EXPERTS, tiles)),
            dma((EXPERTS, tiles)),
            dma((EXPERTS, tiles)),
        ],
        compiler_params=pltpu.CompilerParams(
            collective_id=0, has_side_effects=True, vmem_limit_bytes=VMEM_BYTES
        ),
    )(
        stream[0],
        mixer_gain,
        ssm_weight[0].T,
        decay_rate,
        skip_gain,
        mixed_gain,
        ffn_gain,
        router_weight[0].T,
        expert_ids[0].T,
        gate_weight[0],
        up_weight[0],
        down_weight[0],
    )
    return result[None]


def solution(mesh):
    return jax.shard_map(
        local,
        mesh=mesh,
        in_specs=(
            P("section", "wide", None),
            P("section", None),
            P("section", None, None),
            P("section", None),
            P("section", None),
            P("section", None),
            P("section", None),
            P("section", None, None),
            P("section", "wide", None),
            P("section", None, "wide"),
            P("section", None, "wide"),
            P("section", "wide", None),
        ),
        out_specs=P("section", "wide", None),
        check_vma=False,
    )
```

```python
import functools
import math

import jax
import jax.numpy as jnp
from jax import lax
from jax.experimental import pallas as pl
from jax.experimental.pallas import tpu as pltpu
from jax.sharding import PartitionSpec as P

STATE = 64
EXPERTS = 4
CAP = 40
EPSILON = 1e-05
PIECES = 8
CUTS = 2
LAYERS = 2
VMEM_BYTES = 67_000_000
F32 = jnp.float32
BF16 = jnp.bfloat16


def tile_of(extent, most):
    return max(t for t in range(128, most + 1, 128) if extent % t == 0)


def rms_scale(values, gain_row):
    mean_sq = jnp.mean(values * values, axis=-1, keepdims=True)
    return values * lax.rsqrt(mean_sq + EPSILON) * gain_row


def iota(shape, axis):
    return lax.broadcasted_iota(jnp.int32, shape, axis)


def dot(a, b):
    return jnp.dot(a, b, preferred_element_type=F32)


def split_pair(values):
    high = values.astype(BF16).astype(F32)
    return jnp.concatenate([high, values - high], axis=1)


def tick(
    sections,
    n,
    stream,
    mixer_gain,
    ssm_weight,
    decay_rate,
    skip_gain,
    mixed_gain,
    ffn_gain,
    router_weight,
    expert_ids,
    gate_hbm,
    up_hbm,
    down_hbm,
    out_ref,
    gate,
    up,
    down,
    local_out,
    local_in,
    decay_out,
    decay_in,
    start_out,
    start_in,
    mixed,
    carry,
    resid,
    notes,
    resid_in,
    notes_in,
    packed,
    arrived,
    rows_in,
    hidden,
    answers,
    shared_in,
    totals,
    answers_in,
    picked,
    w_sem,
    local_send,
    local_recv,
    decay_send,
    decay_recv,
    start_send,
    start_recv,
    pass_send,
    pass_recv,
    rows_send,
    rows_recv,
    share_send,
    share_recv,
    ans_send,
    ans_recv,
):
    sec = lax.axis_index("section")
    me = lax.axis_index("wide")
    after = lax.rem(sec + 1, sections)
    before = lax.rem(sec + sections - 1, sections)
    tok, width = stream.shape
    heads = decay_rate.shape[1]
    head_dim = width // heads
    assert tok == head_dim
    chans = width // n
    members = n // EXPERTS
    my_expert, my_part = me // members, lax.rem(me, members)
    hid = gate.shape[1]
    order = [0]
    for k in range(1, n // 2 + 1):
        order += [k] if 2 * k == n else [k, n - k]

    def wide_at(shift):
        return lax.rem(me + (shift + n), n)

    mates = [
        my_expert,
        my_expert + 1 - 2 * lax.rem(my_expert, 2),
        lax.rem(my_expert + 2, EXPERTS),
        EXPERTS - 1 - my_expert,
    ]

    def peer(q, part_shift):
        return mates[q] * members + lax.rem(my_part + (part_shift + members), members)

    def remote(src, dst, send, recv, section, wide):
        return pltpu.make_async_remote_copy(
            src_ref=src,
            dst_ref=dst,
            send_sem=send,
            recv_sem=recv,
            device_id={"section": section, "wide": wide},
            device_id_type=pl.DeviceIdType.MESH,
        )

    barrier = pltpu.get_barrier_semaphore()
    for k in range(n):
        w = wide_at(k)
        if k:
            pl.semaphore_signal(
                barrier, inc=1, device_id={"section": sec, "wide": w},
                device_id_type=pl.DeviceIdType.MESH,
            )
        for other in (after, before):
            pl.semaphore_signal(
                barrier, inc=1, device_id={"section": other, "wide": w},
                device_id_type=pl.DeviceIdType.MESH,
            )

    weight_copies = []
    for i, (src, dst) in enumerate(((gate_hbm, gate), (up_hbm, up), (down_hbm, down))):
        step = src.shape[0] // PIECES
        weight_copies.append(
            [
                pltpu.make_async_copy(
                    src.at[pl.ds(k * step, step)], dst.at[pl.ds(k * step, step)], w_sem.at[i, k]
                )
                for k in range(PIECES)
            ]
        )
        for copy in weight_copies[-1]:
            copy.start()

    x_in = stream[...].astype(F32)
    normed = rms_scale(x_in, mixer_gain[...]).astype(BF16)
    projected = lax.dot_general(
        normed, ssm_weight[...], (((1,), (1,)), ((), ())), preferred_element_type=F32
    )
    raw = projected[:, 2 * STATE :]
    step_size = jnp.maximum(raw, 0.0) + jnp.log1p(jnp.exp(-jnp.abs(raw)))
    b_rows = projected[:, :STATE] * (1.0 / STATE)
    c_rows = (projected[:, STATE : 2 * STATE] * (1.0 / math.sqrt(STATE))).astype(BF16)
    tri = (iota((tok, tok), 0) >= iota((tok, tok), 1)).astype(BF16)
    steps = split_pair(step_size)
    run = dot(tri, steps.astype(BF16))
    rated = (run[:, :heads] + run[:, heads:]) * decay_rate[...]
    skips = jnp.broadcast_to(split_pair(skip_gain[...]), (16, 2 * heads))
    spread = (
        lax.rem(iota((2 * heads, width), 0), heads) == iota((2 * heads, width), 1) // head_dim
    ).astype(BF16)
    cols = dot(
        jnp.concatenate([steps, split_pair(rated), skips], axis=0).astype(BF16), spread
    )
    step_cols, rated_cols = cols[:tok], cols[tok : 2 * tok]
    skip_cols = cols[2 * tok : 2 * tok + 1]
    values = normed.astype(F32)
    scaled = values * step_cols
    last = rated_cols[tok - 1 : tok]

    b_across = jnp.transpose(b_rows).astype(BF16)
    added = dot(b_across, (scaled * jnp.exp(rated_cols - last)).astype(BF16)).astype(BF16)
    faded = jnp.exp(-last)
    depth = STATE // LAYERS
    for j in range(n):
        at = slice(j * chans, (j + 1) * chans)
        decay_out[j] = faded[:, at]
        for s in range(LAYERS):
            local_out[s, j] = added[s * depth : (s + 1) * depth, at]
    pl.semaphore_wait(barrier, 3 * n - 1)
    decay_own = pltpu.make_async_copy(decay_out.at[me], decay_in.at[me], decay_recv.at[me])
    decay_own.start()
    for p in reversed(range(1, n)):
        w = wide_at(order[p])
        remote(
            decay_out.at[w], decay_in.at[me], decay_send.at[w], decay_recv.at[me], sec, w
        ).start()

    def spread_out(s, source, target, send, recv):
        pltpu.make_async_copy(source.at[s, me], target.at[s, me], recv.at[s, me]).start()
        for p in reversed(range(1, n)):
            w = wide_at(order[p])
            remote(
                source.at[s, w], target.at[s, me], send.at[s, w], recv.at[s, me], sec, w
            ).start()

    def collect(s, source, target, send, recv):
        pltpu.make_async_copy(source.at[s, me], target.at[s, me], recv.at[s, me]).wait()
        for p in range(1, n):
            w = wide_at(order[p])
            remote(
                source.at[s, w], target.at[s, w], send.at[s, w], recv.at[s, w], sec, w
            ).wait()

    for s in range(LAYERS):
        spread_out(s, local_out, local_in, local_send, local_recv)

    per = 256 // head_dim
    block = per * head_dim
    b_short = b_rows.astype(BF16)
    overlap = lax.dot_general(
        c_rows, jnp.concatenate([b_rows] * per, axis=0).astype(BF16),
        (((1,), (1,)), ((), ())), preferred_element_type=F32,
    )
    lane_tok = lax.rem(iota((tok, block), 1), tok)
    lane_head = iota((tok, block), 1) // head_dim
    row_tok = iota((tok, block), 0)
    for g in range(width // block):
        at = slice(g * block, (g + 1) * block)
        rated_g, scaled_g = rated_cols[:, at], scaled[:, at]
        rated_row = jnp.sum(
            jnp.where(row_tok == lane_tok, rated_g, 0.0), axis=0, keepdims=True
        )
        gap = jnp.where(row_tok >= lane_tok, rated_row - rated_g, -1e30)
        mixing = (overlap * jnp.exp(gap)).astype(BF16)
        stacked = jnp.concatenate(
            [jnp.where(lane_head == k, scaled_g, 0.0) for k in range(per)], axis=0
        ).astype(BF16)
        mixed[:, at] = dot(mixing, stacked) + values[:, at] * skip_cols[:, at]
        carry[:, at] = jnp.exp(-rated_g)

    decay_own.wait()
    for p in range(1, n):
        w = wide_at(order[p])
        remote(
            decay_out.at[w], decay_in.at[w], decay_send.at[w], decay_recv.at[w], sec, w
        ).wait()
    for s in range(LAYERS):
        collect(s, local_out, local_in, local_send, local_recv)
        state = jnp.zeros((depth, chans), F32)
        for w in range(n):
            start_out[s, w] = state.astype(BF16)
            state = state * decay_in[w] + local_in[s, w].astype(F32)
        spread_out(s, start_out, start_in, start_send, start_recv)

    id_rows = jnp.concatenate([expert_ids[...], jnp.zeros((6, tok), jnp.int32)], axis=0)
    ids = jnp.transpose(id_rows.astype(F32)).astype(jnp.int32)
    id0, id1 = ids[:, 0:1], ids[:, 1:2]
    lane = iota((tok, 128), 1)
    chosen = ((lane == id0) | (lane == id1)).astype(BF16)
    earlier = (iota((tok, tok), 0) > iota((tok, tok), 1)).astype(BF16)
    running = dot(earlier, chosen)
    slot0 = jnp.sum(jnp.where(lane == id0, running, 0.0), axis=1, keepdims=True)
    slot1 = jnp.sum(jnp.where(lane == id1, running, 0.0), axis=1, keepdims=True)
    target0 = id0.astype(F32) * CAP + slot0
    target1 = id1.astype(F32) * CAP + slot1
    places = iota((tok, 256), 1).astype(F32)
    placing = jnp.transpose(((places == target0) | (places == target1)).astype(F32)).astype(BF16)

    for s in range(LAYERS):
        collect(s, start_out, start_in, start_send, start_recv)
    for j in range(n):
        at = slice(j * chans, (j + 1) * chans)
        begun = jnp.concatenate([start_in[s, j] for s in range(LAYERS)], axis=0)
        mixed[:, at] = mixed[:, at] + dot(c_rows, begun) * carry[:, at]
    residual = x_in + rms_scale(mixed[...], mixed_gain[...])
    routed = rms_scale(residual, ffn_gain[...]).astype(BF16)
    sent = dot(placing[: EXPERTS * CAP], routed)
    piece = width // CUTS
    for e in range(EXPERTS):
        for c in range(CUTS):
            packed[e, c] = sent[
                e * CAP : (e + 1) * CAP, c * piece : (c + 1) * piece
            ].astype(BF16)

    row_copies = {}
    rows_own = []
    for c in range(CUTS):
        rows_own.append(
            pltpu.make_async_copy(packed.at[my_expert, c], arrived.at[0, c], rows_recv.at[0, c])
        )
        rows_own[-1].start()

    def hand_on(q, c):
        source = arrived.at[q, c] if q else packed.at[my_expert, c]
        for k in range(1, members):
            p = k * EXPERTS + q
            row_copies[p, c] = remote(
                source, arrived.at[p, c], rows_send.at[p, c], rows_recv.at[p, c], sec, peer(0, -k)
            )
            row_copies[p, c].start()

    for c in range(CUTS):
        hand_on(0, c)
    for q in (2, 1, 3):
        for c in range(CUTS):
            row_copies[q, c] = remote(
                packed.at[mates[q], c], arrived.at[q, c], rows_send.at[q, c], rows_recv.at[q, c],
                sec, peer(q, 0),
            )
            row_copies[q, c].start()

    logits = lax.dot_general(
        routed, router_weight[...], (((1,), (1,)), ((), ())), preferred_element_type=F32
    )
    choice = iota((tok, EXPERTS), 1)
    logit0 = jnp.sum(jnp.where(choice == id0, logits, 0.0), axis=1, keepdims=True)
    logit1 = jnp.sum(jnp.where(choice == id1, logits, 0.0), axis=1, keepdims=True)
    share0 = jax.nn.sigmoid(logit0 - logit1)
    resid[...] = residual
    notes[...] = jnp.where(
        lane == 0, target0, jnp.where(lane == 1, target1, jnp.where(lane == 2, share0, 0.0))
    )
    passes = [
        remote(resid, resid_in, pass_send.at[0], pass_recv.at[0], after, me),
        remote(notes, notes_in, pass_send.at[1], pass_recv.at[1], after, me),
    ]
    for copy in passes:
        copy.start()

    def relay(q, c):
        row_copies[q, c].wait_recv()
        hand_on(q, c)

    hid_tile = tile_of(hid, 512)
    out_tile = totals.shape[3]
    tiles = width // out_tile
    steps_up = hid // hid_tile
    groups = ((0, 2), (1, 3))
    half = n // 2
    share_copies = {}
    answer_copies = {}

    def gather(group):
        block_at = 0
        for k in range(members):
            for q in groups[group]:
                p = k * EXPERTS + q
                for c in range(CUTS):
                    if p == 0:
                        rows_own[c].wait()
                    elif k:
                        row_copies[p, c].wait_recv()
                block_at += 1
            lead = k * EXPERTS + groups[group][0]
            other = k * EXPERTS + groups[group][1]
            top = k * 2 * CAP
            for c in range(CUTS):
                rows_in[top : top + 2 * CAP, c * piece : (c + 1) * piece] = jnp.concatenate(
                    [arrived[lead, c].astype(F32), arrived[other, c].astype(F32)], axis=0
                ).astype(BF16)

    def widen_span(first, beyond):
        @pl.loop(first, beyond)
        def _(i):
            at = pl.ds(pl.multiple_of(i * hid_tile, hid_tile), hid_tile)
            gate_pre = dot(rows_in[...], gate[:, at])
            up_pre = dot(rows_in[...], up[:, at])
            hidden[:, at] = (gate_pre * jax.nn.sigmoid(gate_pre) * up_pre).astype(BF16)

    def widen(hooks):
        done = 0
        for share, action in hooks:
            upto = int(steps_up * share)
            if upto > done:
                widen_span(done, upto)
            action()
            done = max(done, upto)
        if done < steps_up:
            widen_span(done, steps_up)

    def narrow(group):
        for i in range(tiles):
            result = dot(hidden[...], down[:, i * out_tile : (i + 1) * out_tile])
            for k in reversed(range(members)):
                for h, q in enumerate(groups[group]):
                    p = k * EXPERTS + q
                    top = (k * 2 + h) * CAP
                    answers[p, i] = result[top : top + CAP].astype(BF16)
            for k in range(1, members):
                for q in groups[group]:
                    p = k * EXPERTS + q
                    share_copies[p, i] = remote(
                        answers.at[p, i], shared_in.at[p - EXPERTS, i],
                        share_send.at[p - EXPERTS, i], share_recv.at[p - EXPERTS, i],
                        sec, peer(0, k),
                    )
                    share_copies[p, i].start()

    def settle(group, i):
        for q in reversed(groups[group]):
            total = answers[q, i].astype(F32)
            for k in range(1, members):
                p = k * EXPERTS + q
                share_copies[p, i].wait_recv()
                total = total + shared_in[p - EXPERTS, i].astype(F32)
            totals[q, i] = total.astype(BF16)
            answer_copies[q, i] = remote(
                totals.at[q, i], answers_in.at[q, i], ans_send.at[q, i], ans_recv.at[q, i],
                after, peer(q, 0),
            )
            answer_copies[q, i].start()

    for q in (2, 1):
        for c in range(CUTS):
            relay(q, c)
    gather(0)
    for copies in weight_copies[:2]:
        for copy in copies:
            copy.wait()
    widen([((2 + c) / (2 + CUTS), functools.partial(relay, 3, c)) for c in range(CUTS)])
    for copy in weight_copies[2]:
        copy.wait()
    narrow(0)
    gather(1)
    widen([((2 + 2 * i / (tiles - 1)) / 4, functools.partial(settle, 0, i)) for i in range(tiles)])
    narrow(1)

    for copy in passes:
        copy.wait()
    told = notes_in[...]
    goal0, goal1, first_share = told[:, 0:1], told[:, 1:2], told[:, 2:3]
    slot_lane = iota((tok, CAP), 1)

    def take(q):
        spots = (slot_lane + mates[q] * CAP).astype(F32)
        return jnp.concatenate(
            [(spots == goal0).astype(F32), (spots == goal1).astype(F32)], axis=0
        ).astype(BF16)

    for i in range(tiles):
        settle(1, i)
    takes = [take(q) for q in range(EXPERTS)]
    for i in range(tiles):
        at = slice(i * out_tile, (i + 1) * out_tile)
        found = None
        for q in groups[0]:
            answer_copies[q, i].wait_recv()
            part = dot(takes[q], answers_in[q, i])
            found = part if found is None else found + part
        picked[:, at] = found
    for i in range(tiles):
        at = slice(i * out_tile, (i + 1) * out_tile)
        found = picked[:, at]
        for q in groups[1]:
            answer_copies[q, i].wait_recv()
            found = found + dot(takes[q], answers_in[q, i])
        out_ref[:, at] = (
            resid_in[:, at] + (first_share * found[:tok] + (1.0 - first_share) * found[tok:])
        ).astype(BF16)
    for p in range(1, n):
        for c in range(CUTS):
            row_copies[p, c].wait_send()
    for copy in share_copies.values():
        copy.wait_send()
    for copy in answer_copies.values():
        copy.wait_send()


def local(
    stream,
    mixer_gain,
    ssm_weight,
    decay_rate,
    skip_gain,
    mixed_gain,
    ffn_gain,
    router_weight,
    expert_ids,
    gate_weight,
    up_weight,
    down_weight,
):
    n = lax.axis_size("wide")
    sections = lax.axis_size("section")
    _, tok, width = stream.shape
    hid = gate_weight.shape[2]
    chans = width // n
    out_tile = tile_of(width, 512)
    tiles = width // out_tile
    dma = pltpu.SemaphoreType.DMA
    vmem = pl.BlockSpec(memory_space=pltpu.VMEM)
    hbm = pl.BlockSpec(memory_space=pl.ANY)
    result = pl.pallas_call(
        functools.partial(tick, sections, n),
        out_shape=jax.ShapeDtypeStruct((tok, width), BF16),
        in_specs=[vmem] * 9 + [hbm] * 3,
        out_specs=vmem,
        scratch_shapes=[
            pltpu.VMEM((width, hid), BF16),
            pltpu.VMEM((width, hid), BF16),
            pltpu.VMEM((hid, width), BF16),
            pltpu.VMEM((LAYERS, n, STATE // LAYERS, chans), BF16),
            pltpu.VMEM((LAYERS, n, STATE // LAYERS, chans), BF16),
            pltpu.VMEM((n, 1, chans), F32),
            pltpu.VMEM((n, 1, chans), F32),
            pltpu.VMEM((LAYERS, n, STATE // LAYERS, chans), BF16),
            pltpu.VMEM((LAYERS, n, STATE // LAYERS, chans), BF16),
            pltpu.VMEM((tok, width), F32),
            pltpu.VMEM((tok, width), F32),
            pltpu.VMEM((tok, width), F32),
            pltpu.VMEM((tok, 128), F32),
            pltpu.VMEM((tok, width), F32),
            pltpu.VMEM((tok, 128), F32),
            pltpu.VMEM((EXPERTS, CUTS, CAP, width // CUTS), BF16),
            pltpu.VMEM((n, CUTS, CAP, width // CUTS), BF16),
            pltpu.VMEM((n // 2 * CAP, width), BF16),
            pltpu.VMEM((n // 2 * CAP, hid), BF16),
            pltpu.VMEM((n, tiles, CAP, out_tile), BF16),
            pltpu.VMEM((n - EXPERTS, tiles, CAP, out_tile), BF16),
            pltpu.VMEM((EXPERTS, tiles, CAP, out_tile), BF16),
            pltpu.VMEM((EXPERTS, tiles, CAP, out_tile), BF16),
            pltpu.VMEM((2 * tok, width), F32),
            dma((3, PIECES)),
            dma((LAYERS, n)),
            dma((LAYERS, n)),
            dma((n,)),
            dma((n,)),
            dma((LAYERS, n)),
            dma((LAYERS, n)),
            dma((2,)),
            dma((2,)),
            dma((n, CUTS)),
            dma((n, CUTS)),
            dma((n - EXPERTS, tiles)),
            dma((n - EXPERTS, tiles)),
            dma((EXPERTS, tiles)),
            dma((EXPERTS, tiles)),
        ],
        compiler_params=pltpu.CompilerParams(
            collective_id=0, has_side_effects=True, vmem_limit_bytes=VMEM_BYTES
        ),
    )(
        stream[0],
        mixer_gain,
        ssm_weight[0].T,
        decay_rate,
        skip_gain,
        mixed_gain,
        ffn_gain,
        router_weight[0].T,
        expert_ids[0].T,
        gate_weight[0],
        up_weight[0],
        down_weight[0],
    )
    return result[None]


def solution(mesh):
    return jax.shard_map(
        local,
        mesh=mesh,
        in_specs=(
            P("section", "wide", None),
            P("section", None),
            P("section", None, None),
            P("section", None),
            P("section", None),
            P("section", None),
            P("section", None),
            P("section", None, None),
            P("section", "wide", None),
            P("section", None, "wide"),
            P("section", None, "wide"),
            P("section", "wide", None),
        ),
        out_specs=P("section", "wide", None),
        check_vma=False,
    )
```

```python
import functools
import math

import jax
import jax.numpy as jnp
from jax import lax
from jax.experimental import pallas as pl
from jax.experimental.pallas import tpu as pltpu
from jax.sharding import PartitionSpec as P

STATE = 64
EXPERTS = 4
CAP = 40
EPSILON = 1e-05
PIECES = 8
CUTS = 2
LAYERS = 2
VMEM_BYTES = 67_000_000
F32 = jnp.float32
BF16 = jnp.bfloat16


def tile_of(extent, most):
    return max(t for t in range(128, most + 1, 128) if extent % t == 0)


def rms_scale(values, gain_row):
    mean_sq = jnp.mean(values * values, axis=-1, keepdims=True)
    return values * lax.rsqrt(mean_sq + EPSILON) * gain_row


def iota(shape, axis):
    return lax.broadcasted_iota(jnp.int32, shape, axis)


def dot(a, b):
    return jnp.dot(a, b, preferred_element_type=F32)


def split_pair(values):
    high = values.astype(BF16).astype(F32)
    return jnp.concatenate([high, values - high], axis=1)


def tick(
    sections,
    n,
    stream,
    mixer_gain,
    ssm_weight,
    decay_rate,
    skip_gain,
    mixed_gain,
    ffn_gain,
    router_weight,
    expert_ids,
    gate_hbm,
    up_hbm,
    down_hbm,
    out_ref,
    gate,
    up,
    down,
    local_out,
    local_in,
    decay_out,
    decay_in,
    start_out,
    start_in,
    mixed,
    carry,
    resid,
    notes,
    resid_in,
    notes_in,
    packed,
    arrived,
    rows_in,
    hidden,
    answers,
    shared_in,
    totals,
    answers_in,
    picked,
    finished,
    w_sem,
    local_send,
    local_recv,
    decay_send,
    decay_recv,
    start_send,
    start_recv,
    pass_send,
    pass_recv,
    rows_send,
    rows_recv,
    share_send,
    share_recv,
    ans_send,
    ans_recv,
    out_sem,
):
    sec = lax.axis_index("section")
    me = lax.axis_index("wide")
    after = lax.rem(sec + 1, sections)
    before = lax.rem(sec + sections - 1, sections)
    tok, width = stream.shape
    heads = decay_rate.shape[1]
    head_dim = width // heads
    assert tok == head_dim
    chans = width // n
    members = n // EXPERTS
    my_expert, my_part = me // members, lax.rem(me, members)
    hid = gate.shape[1]
    order = [0]
    for k in range(1, n // 2 + 1):
        order += [k] if 2 * k == n else [k, n - k]

    def wide_at(shift):
        return lax.rem(me + (shift + n), n)

    mates = [
        my_expert,
        my_expert + 1 - 2 * lax.rem(my_expert, 2),
        lax.rem(my_expert + 2, EXPERTS),
        EXPERTS - 1 - my_expert,
    ]

    def peer(q, part_shift):
        return mates[q] * members + lax.rem(my_part + (part_shift + members), members)

    def remote(src, dst, send, recv, section, wide):
        return pltpu.make_async_remote_copy(
            src_ref=src,
            dst_ref=dst,
            send_sem=send,
            recv_sem=recv,
            device_id={"section": section, "wide": wide},
            device_id_type=pl.DeviceIdType.MESH,
        )

    barrier = pltpu.get_barrier_semaphore()
    for k in range(n):
        w = wide_at(k)
        if k:
            pl.semaphore_signal(
                barrier, inc=1, device_id={"section": sec, "wide": w},
                device_id_type=pl.DeviceIdType.MESH,
            )
        for other in (after, before):
            pl.semaphore_signal(
                barrier, inc=1, device_id={"section": other, "wide": w},
                device_id_type=pl.DeviceIdType.MESH,
            )

    weight_copies = []
    for i, (src, dst) in enumerate(((gate_hbm, gate), (up_hbm, up), (down_hbm, down))):
        step = src.shape[0] // PIECES
        weight_copies.append(
            [
                pltpu.make_async_copy(
                    src.at[pl.ds(k * step, step)], dst.at[pl.ds(k * step, step)], w_sem.at[i, k]
                )
                for k in range(PIECES)
            ]
        )
        for copy in weight_copies[-1]:
            copy.start()

    x_in = stream[...].astype(F32)
    normed = rms_scale(x_in, mixer_gain[...]).astype(BF16)
    projected = lax.dot_general(
        normed, ssm_weight[...], (((1,), (1,)), ((), ())), preferred_element_type=F32
    )
    raw = projected[:, 2 * STATE :]
    step_size = jnp.maximum(raw, 0.0) + jnp.log1p(jnp.exp(-jnp.abs(raw)))
    b_rows = projected[:, :STATE] * (1.0 / STATE)
    c_rows = (projected[:, STATE : 2 * STATE] * (1.0 / math.sqrt(STATE))).astype(BF16)
    tri = (iota((tok, tok), 0) >= iota((tok, tok), 1)).astype(BF16)
    steps = split_pair(step_size)
    run = dot(tri, steps.astype(BF16))
    rated = (run[:, :heads] + run[:, heads:]) * decay_rate[...]
    skips = jnp.broadcast_to(split_pair(skip_gain[...]), (16, 2 * heads))
    spread = (
        lax.rem(iota((2 * heads, width), 0), heads) == iota((2 * heads, width), 1) // head_dim
    ).astype(BF16)
    cols = dot(
        jnp.concatenate([steps, split_pair(rated), skips], axis=0).astype(BF16), spread
    )
    step_cols, rated_cols = cols[:tok], cols[tok : 2 * tok]
    skip_cols = cols[2 * tok : 2 * tok + 1]
    values = normed.astype(F32)
    scaled = values * step_cols
    last = rated_cols[tok - 1 : tok]

    b_across = jnp.transpose(b_rows).astype(BF16)
    added = dot(b_across, (scaled * jnp.exp(rated_cols - last)).astype(BF16)).astype(BF16)
    faded = jnp.exp(-last)
    depth = STATE // LAYERS
    for j in range(n):
        at = slice(j * chans, (j + 1) * chans)
        decay_out[j] = faded[:, at]
        for s in range(LAYERS):
            local_out[s, j] = added[s * depth : (s + 1) * depth, at]
    pl.semaphore_wait(barrier, 3 * n - 1)
    decay_own = pltpu.make_async_copy(decay_out.at[me], decay_in.at[me], decay_recv.at[me])
    decay_own.start()
    for p in reversed(range(1, n)):
        w = wide_at(order[p])
        remote(
            decay_out.at[w], decay_in.at[me], decay_send.at[w], decay_recv.at[me], sec, w
        ).start()

    def spread_out(s, source, target, send, recv):
        pltpu.make_async_copy(source.at[s, me], target.at[s, me], recv.at[s, me]).start()
        for p in reversed(range(1, n)):
            w = wide_at(order[p])
            remote(
                source.at[s, w], target.at[s, me], send.at[s, w], recv.at[s, me], sec, w
            ).start()

    def collect(s, source, target, send, recv):
        pltpu.make_async_copy(source.at[s, me], target.at[s, me], recv.at[s, me]).wait()
        for p in range(1, n):
            w = wide_at(order[p])
            remote(
                source.at[s, w], target.at[s, w], send.at[s, w], recv.at[s, w], sec, w
            ).wait()

    for s in range(LAYERS):
        spread_out(s, local_out, local_in, local_send, local_recv)

    per = 256 // head_dim
    block = per * head_dim
    b_short = b_rows.astype(BF16)
    overlap = lax.dot_general(
        c_rows, jnp.concatenate([b_rows] * per, axis=0).astype(BF16),
        (((1,), (1,)), ((), ())), preferred_element_type=F32,
    )
    lane_tok = lax.rem(iota((tok, block), 1), tok)
    lane_head = iota((tok, block), 1) // head_dim
    row_tok = iota((tok, block), 0)
    for g in range(width // block):
        at = slice(g * block, (g + 1) * block)
        rated_g, scaled_g = rated_cols[:, at], scaled[:, at]
        rated_row = jnp.sum(
            jnp.where(row_tok == lane_tok, rated_g, 0.0), axis=0, keepdims=True
        )
        gap = jnp.where(row_tok >= lane_tok, rated_row - rated_g, -1e30)
        mixing = (overlap * jnp.exp(gap)).astype(BF16)
        stacked = jnp.concatenate(
            [jnp.where(lane_head == k, scaled_g, 0.0) for k in range(per)], axis=0
        ).astype(BF16)
        mixed[:, at] = dot(mixing, stacked) + values[:, at] * skip_cols[:, at]
        carry[:, at] = jnp.exp(-rated_g)

    decay_own.wait()
    for p in range(1, n):
        w = wide_at(order[p])
        remote(
            decay_out.at[w], decay_in.at[w], decay_send.at[w], decay_recv.at[w], sec, w
        ).wait()
    for s in range(LAYERS):
        collect(s, local_out, local_in, local_send, local_recv)
        state = jnp.zeros((depth, chans), F32)
        for w in range(n):
            start_out[s, w] = state.astype(BF16)
            state = state * decay_in[w] + local_in[s, w].astype(F32)
        spread_out(s, start_out, start_in, start_send, start_recv)

    id_rows = jnp.concatenate([expert_ids[...], jnp.zeros((6, tok), jnp.int32)], axis=0)
    ids = jnp.transpose(id_rows.astype(F32)).astype(jnp.int32)
    id0, id1 = ids[:, 0:1], ids[:, 1:2]
    lane = iota((tok, 128), 1)
    chosen = ((lane == id0) | (lane == id1)).astype(BF16)
    earlier = (iota((tok, tok), 0) > iota((tok, tok), 1)).astype(BF16)
    running = dot(earlier, chosen)
    slot0 = jnp.sum(jnp.where(lane == id0, running, 0.0), axis=1, keepdims=True)
    slot1 = jnp.sum(jnp.where(lane == id1, running, 0.0), axis=1, keepdims=True)
    target0 = id0.astype(F32) * CAP + slot0
    target1 = id1.astype(F32) * CAP + slot1
    places = iota((tok, 256), 1).astype(F32)
    placing = jnp.transpose(((places == target0) | (places == target1)).astype(F32)).astype(BF16)

    for s in range(LAYERS):
        collect(s, start_out, start_in, start_send, start_recv)
    for j in range(n):
        at = slice(j * chans, (j + 1) * chans)
        begun = jnp.concatenate([start_in[s, j] for s in range(LAYERS)], axis=0)
        mixed[:, at] = mixed[:, at] + dot(c_rows, begun) * carry[:, at]
    residual = x_in + rms_scale(mixed[...], mixed_gain[...])
    routed = rms_scale(residual, ffn_gain[...]).astype(BF16)
    sent = dot(placing[: EXPERTS * CAP], routed)
    piece = width // CUTS
    for e in range(EXPERTS):
        for c in range(CUTS):
            packed[e, c] = sent[
                e * CAP : (e + 1) * CAP, c * piece : (c + 1) * piece
            ].astype(BF16)

    row_copies = {}
    rows_own = []
    for c in range(CUTS):
        rows_own.append(
            pltpu.make_async_copy(packed.at[my_expert, c], arrived.at[0, c], rows_recv.at[0, c])
        )
        rows_own[-1].start()

    def hand_on(q, c):
        source = arrived.at[q, c] if q else packed.at[my_expert, c]
        for k in range(1, members):
            p = k * EXPERTS + q
            row_copies[p, c] = remote(
                source, arrived.at[p, c], rows_send.at[p, c], rows_recv.at[p, c], sec, peer(0, -k)
            )
            row_copies[p, c].start()

    for c in range(CUTS):
        hand_on(0, c)
    for q in (2, 1, 3):
        for c in range(CUTS):
            row_copies[q, c] = remote(
                packed.at[mates[q], c], arrived.at[q, c], rows_send.at[q, c], rows_recv.at[q, c],
                sec, peer(q, 0),
            )
            row_copies[q, c].start()

    logits = lax.dot_general(
        routed, router_weight[...], (((1,), (1,)), ((), ())), preferred_element_type=F32
    )
    choice = iota((tok, EXPERTS), 1)
    logit0 = jnp.sum(jnp.where(choice == id0, logits, 0.0), axis=1, keepdims=True)
    logit1 = jnp.sum(jnp.where(choice == id1, logits, 0.0), axis=1, keepdims=True)
    share0 = jax.nn.sigmoid(logit0 - logit1)
    resid[...] = residual
    notes[...] = jnp.where(
        lane == 0, target0, jnp.where(lane == 1, target1, jnp.where(lane == 2, share0, 0.0))
    )
    passes = [
        remote(resid, resid_in, pass_send.at[0], pass_recv.at[0], after, me),
        remote(notes, notes_in, pass_send.at[1], pass_recv.at[1], after, me),
    ]
    for copy in passes:
        copy.start()

    def relay(q, c):
        row_copies[q, c].wait_recv()
        hand_on(q, c)

    hid_tile = tile_of(hid, 512)
    out_tile = totals.shape[3]
    tiles = width // out_tile
    steps_up = hid // hid_tile
    groups = ((0, 2), (1, 3))
    half = n // 2
    share_copies = {}
    answer_copies = {}

    def gather(group):
        block_at = 0
        for k in range(members):
            for q in groups[group]:
                p = k * EXPERTS + q
                for c in range(CUTS):
                    if p == 0:
                        rows_own[c].wait()
                    elif k:
                        row_copies[p, c].wait_recv()
                block_at += 1
            lead = k * EXPERTS + groups[group][0]
            other = k * EXPERTS + groups[group][1]
            top = k * 2 * CAP
            for c in range(CUTS):
                rows_in[top : top + 2 * CAP, c * piece : (c + 1) * piece] = jnp.concatenate(
                    [arrived[lead, c].astype(F32), arrived[other, c].astype(F32)], axis=0
                ).astype(BF16)

    def widen_span(first, beyond):
        @pl.loop(first, beyond)
        def _(i):
            at = pl.ds(pl.multiple_of(i * hid_tile, hid_tile), hid_tile)
            gate_pre = dot(rows_in[...], gate[:, at])
            up_pre = dot(rows_in[...], up[:, at])
            hidden[:, at] = (gate_pre * jax.nn.sigmoid(gate_pre) * up_pre).astype(BF16)

    def widen(hooks):
        done = 0
        for share, action in hooks:
            upto = int(steps_up * share)
            if upto > done:
                widen_span(done, upto)
            action()
            done = max(done, upto)
        if done < steps_up:
            widen_span(done, steps_up)

    def narrow(group):
        for i in range(tiles):
            result = dot(hidden[...], down[:, i * out_tile : (i + 1) * out_tile])
            for k in reversed(range(members)):
                for h, q in enumerate(groups[group]):
                    p = k * EXPERTS + q
                    top = (k * 2 + h) * CAP
                    answers[p, i] = result[top : top + CAP].astype(BF16)
            for k in range(1, members):
                for q in groups[group]:
                    p = k * EXPERTS + q
                    share_copies[p, i] = remote(
                        answers.at[p, i], shared_in.at[p - EXPERTS, i],
                        share_send.at[p - EXPERTS, i], share_recv.at[p - EXPERTS, i],
                        sec, peer(0, k),
                    )
                    share_copies[p, i].start()

    def settle(group, i):
        for q in reversed(groups[group]):
            total = answers[q, i].astype(F32)
            for k in range(1, members):
                p = k * EXPERTS + q
                share_copies[p, i].wait_recv()
                total = total + shared_in[p - EXPERTS, i].astype(F32)
            totals[q, i] = total.astype(BF16)
            answer_copies[q, i] = remote(
                totals.at[q, i], answers_in.at[q, i], ans_send.at[q, i], ans_recv.at[q, i],
                after, peer(q, 0),
            )
            answer_copies[q, i].start()

    for q in (2, 1):
        for c in range(CUTS):
            relay(q, c)
    gather(0)
    for copies in weight_copies[:2]:
        for copy in copies:
            copy.wait()
    widen([((2 + c) / (2 + CUTS), functools.partial(relay, 3, c)) for c in range(CUTS)])
    for copy in weight_copies[2]:
        copy.wait()
    narrow(0)
    gather(1)
    widen([((2 + 2 * i / (tiles - 1)) / 4, functools.partial(settle, 0, i)) for i in range(tiles)])
    narrow(1)

    for copy in passes:
        copy.wait()
    told = notes_in[...]
    goal0, goal1, first_share = told[:, 0:1], told[:, 1:2], told[:, 2:3]
    slot_lane = iota((tok, CAP), 1)

    def take(q):
        spots = (slot_lane + mates[q] * CAP).astype(F32)
        return jnp.concatenate(
            [(spots == goal0).astype(F32), (spots == goal1).astype(F32)], axis=0
        ).astype(BF16)

    for i in range(tiles):
        settle(1, i)
    takes = [take(q) for q in range(EXPERTS)]
    for i in range(tiles):
        at = slice(i * out_tile, (i + 1) * out_tile)
        found = None
        for q in groups[0]:
            answer_copies[q, i].wait_recv()
            part = dot(takes[q], answers_in[q, i])
            found = part if found is None else found + part
        picked[:, at] = found
    out_copies = []
    for i in range(tiles):
        at = slice(i * out_tile, (i + 1) * out_tile)
        found = picked[:, at]
        for q in groups[1]:
            answer_copies[q, i].wait_recv()
            found = found + dot(takes[q], answers_in[q, i])
        finished[:, at] = (
            resid_in[:, at] + (first_share * found[:tok] + (1.0 - first_share) * found[tok:])
        ).astype(BF16)
        out_copies.append(
            pltpu.make_async_copy(finished.at[:, at], out_ref.at[:, at], out_sem.at[i])
        )
        out_copies[-1].start()
    for p in range(1, n):
        for c in range(CUTS):
            row_copies[p, c].wait_send()
    for copy in share_copies.values():
        copy.wait_send()
    for copy in answer_copies.values():
        copy.wait_send()
    for copy in out_copies:
        copy.wait()


def local(
    stream,
    mixer_gain,
    ssm_weight,
    decay_rate,
    skip_gain,
    mixed_gain,
    ffn_gain,
    router_weight,
    expert_ids,
    gate_weight,
    up_weight,
    down_weight,
):
    n = lax.axis_size("wide")
    sections = lax.axis_size("section")
    _, tok, width = stream.shape
    hid = gate_weight.shape[2]
    chans = width // n
    out_tile = tile_of(width, 512)
    tiles = width // out_tile
    dma = pltpu.SemaphoreType.DMA
    vmem = pl.BlockSpec(memory_space=pltpu.VMEM)
    hbm = pl.BlockSpec(memory_space=pl.ANY)
    result = pl.pallas_call(
        functools.partial(tick, sections, n),
        out_shape=jax.ShapeDtypeStruct((tok, width), BF16),
        in_specs=[vmem] * 9 + [hbm] * 3,
        out_specs=hbm,
        scratch_shapes=[
            pltpu.VMEM((width, hid), BF16),
            pltpu.VMEM((width, hid), BF16),
            pltpu.VMEM((hid, width), BF16),
            pltpu.VMEM((LAYERS, n, STATE // LAYERS, chans), BF16),
            pltpu.VMEM((LAYERS, n, STATE // LAYERS, chans), BF16),
            pltpu.VMEM((n, 1, chans), F32),
            pltpu.VMEM((n, 1, chans), F32),
            pltpu.VMEM((LAYERS, n, STATE // LAYERS, chans), BF16),
            pltpu.VMEM((LAYERS, n, STATE // LAYERS, chans), BF16),
            pltpu.VMEM((tok, width), F32),
            pltpu.VMEM((tok, width), F32),
            pltpu.VMEM((tok, width), F32),
            pltpu.VMEM((tok, 128), F32),
            pltpu.VMEM((tok, width), F32),
            pltpu.VMEM((tok, 128), F32),
            pltpu.VMEM((EXPERTS, CUTS, CAP, width // CUTS), BF16),
            pltpu.VMEM((n, CUTS, CAP, width // CUTS), BF16),
            pltpu.VMEM((n // 2 * CAP, width), BF16),
            pltpu.VMEM((n // 2 * CAP, hid), BF16),
            pltpu.VMEM((n, tiles, CAP, out_tile), BF16),
            pltpu.VMEM((n - EXPERTS, tiles, CAP, out_tile), BF16),
            pltpu.VMEM((EXPERTS, tiles, CAP, out_tile), BF16),
            pltpu.VMEM((EXPERTS, tiles, CAP, out_tile), BF16),
            pltpu.VMEM((2 * tok, width), F32),
            pltpu.VMEM((tok, width), BF16),
            dma((3, PIECES)),
            dma((LAYERS, n)),
            dma((LAYERS, n)),
            dma((n,)),
            dma((n,)),
            dma((LAYERS, n)),
            dma((LAYERS, n)),
            dma((2,)),
            dma((2,)),
            dma((n, CUTS)),
            dma((n, CUTS)),
            dma((n - EXPERTS, tiles)),
            dma((n - EXPERTS, tiles)),
            dma((EXPERTS, tiles)),
            dma((EXPERTS, tiles)),
            dma((tiles,)),
        ],
        compiler_params=pltpu.CompilerParams(
            collective_id=0, has_side_effects=True, vmem_limit_bytes=VMEM_BYTES
        ),
    )(
        stream[0],
        mixer_gain,
        ssm_weight[0].T,
        decay_rate,
        skip_gain,
        mixed_gain,
        ffn_gain,
        router_weight[0].T,
        expert_ids[0].T,
        gate_weight[0],
        up_weight[0],
        down_weight[0],
    )
    return result[None]


def solution(mesh):
    return jax.shard_map(
        local,
        mesh=mesh,
        in_specs=(
            P("section", "wide", None),
            P("section", None),
            P("section", None, None),
            P("section", None),
            P("section", None),
            P("section", None),
            P("section", None),
            P("section", None, None),
            P("section", "wide", None),
            P("section", None, "wide"),
            P("section", None, "wide"),
            P("section", "wide", None),
        ),
        out_specs=P("section", "wide", None),
        check_vma=False,
    )
```
